128 devices in a mesh: gx: 16 (over y_lo, x, core), gy: 8 (over z, y_hi).
Axes of the slice: x: 4, y: 4 (y_hi: 2, y_lo: 2; y = y_hi * 2 + y_lo), z: 4, core: 2. Of those that a mesh axis runs over, the one named last changes fastest.
Arguments:
- features: bfloat16 [65536, 128], P(('gx', 'gy')), may hold values from -6 to 6
- cache_in: bfloat16 [65536, 128], replicated, may hold values from -26 to 26
- cache_hidden: bfloat16 [65536, 128], replicated, may hold values from -26 to 26
- tiles: bfloat16 [128, 128, 256, 256], P(('gx', 'gy')), may hold values from -0.03125 to 0.03125
- tile_pos: int32 [128, 128, 2], P(('gx', 'gy')), may hold values from 0 to 1
- order: int32 [2, 128], replicated, may hold values from 0 to 127, each once within a row
- skip: int32 [2, 128], replicated, may hold values 0 or 1
- w_first: bfloat16 [128, 128], replicated, may hold values from -0.5 to 0.5
- w_second: bfloat16 [128, 128], replicated, may hold values from -0.5 to 0.5
Outputs:
- output: bfloat16 [65536, 128], P(('gx', 'gy'))
- drift: float32 [2], replicated
The draws below stay inside these ranges and needn't reach their ends.
Inputs may be any that keep to these rules, and one draw needn't show every extreme that they name: `order`: each row names every block once.
All inputs are finite; a program needn't handle non-finite values.
Results may differ from the reference program's by a relative error of at most 0.0052.
Values may be sent and summed in bfloat16 or wider, within the bound.
No kernel may reach another device: no remote copies, remote signals or barrier semaphores. Data moves between devices by JAX's collectives and lax.ppermute only.
A program may use at most 192 MiB of HBM per device.

```python
import jax
import jax.numpy as jnp
from jax import lax

F = 128
HID = 128
V_DEV = 512
NB = 128
TS = 256
V = 65536


def scaled_rows(key, width):
    total_rows = NB * V_DEV
    position = jnp.arange(total_rows, dtype=jnp.float32) / max(total_rows - 1, 1)
    noise = jnp.clip(jax.random.normal(key, (total_rows, width), jnp.float32), -6.0, 6.0)
    row_scale = 0.5 + 1.5 * position
    values = row_scale[:, None] * noise
    return values.astype(jnp.bfloat16)


def draw_cache_in(key, part):
    return scaled_rows(jax.random.fold_in(key, 11), F)


def draw_cache_hidden(key, part):
    return scaled_rows(jax.random.fold_in(key, 23), HID)


def plant(entries, key, least, high):
    place = [jax.random.randint(jax.random.fold_in(key, axis), (), 0, length) for axis, length in enumerate(entries.shape)]
    main_axis = entries.shape.index(max(entries.shape))
    next_to = place[:main_axis] + [(place[main_axis] + 1) % entries.shape[main_axis]] + place[main_axis + 1:]
    return entries.at[tuple(place)].set(least).at[tuple(next_to)].set(high)


def levels(stream_key, shape, cuts, least, high):
    def one(dim, shards_of):
        draws = jax.random.uniform(jax.random.fold_in(jax.random.fold_in(stream_key, 6), dim), (shards_of,), jnp.float32, least / len(cuts), high / len(cuts))
        return jnp.repeat(jnp.exp(draws), shape[dim] // shards_of).reshape((-1,) + (1,) * (len(shape) - dim - 1))

    loudness = one(*cuts[0])
    for cut in cuts[1:]:
        loudness = loudness * one(*cut)
    return loudness


def bell_draw(stream_key, extent, scale, most, pieces=(), kind=jnp.bfloat16):
    entries = scale * jax.random.normal(stream_key, extent, jnp.float32)
    if pieces:
        entries = entries * levels(stream_key, extent, pieces, -0.22, 0.18)
    return jnp.clip(entries, -most, most).astype(kind)


def setup_inputs(seed: int = 0) -> dict:
    seeds = jax.random.split(jax.random.key(seed), 10)
    features = bell_draw(seeds[0], (V, F), 1.0, 6.0, ((0, 128),))
    cache_in = draw_cache_in(jax.random.fold_in(seeds[9], 71), 0)
    cache_hidden = draw_cache_hidden(jax.random.fold_in(seeds[9], 71), 0)
    tiles = bell_draw(seeds[3], (NB, NB, TS, TS), (NB * TS) ** -0.5, 0.03125, ((0, 128),))
    tile_pos = plant(jax.random.randint(seeds[4], (NB, NB, 2), 0, 2), jax.random.fold_in(seeds[4], 1), 0, 1).astype(jnp.int32)
    order = jax.vmap(lambda own: jax.random.permutation(own, NB))(jax.random.split(seeds[5], 2)).reshape((2, NB)).astype(jnp.int32)
    skip = plant((jax.random.randint(seeds[6], (2, NB), 0, 2) < 1).astype(jnp.int32), jax.random.fold_in(seeds[6], 1), 0, 1)
    w_first = bell_draw(seeds[7], (F, HID), F ** -0.5, 0.5)
    w_second = bell_draw(seeds[8], (HID, HID), HID ** -0.5, 0.5)
    return {"features": features, "cache_in": cache_in, "cache_hidden": cache_hidden, "tiles": tiles, "tile_pos": tile_pos, "order": order, "skip": skip, "w_first": w_first, "w_second": w_second}


def refreshed_flags(order, skip):
    round_hits = (order[:, :, None] == jnp.arange(NB, dtype=jnp.int32)[None, None, :]).astype(jnp.int32)
    return jnp.sum(round_hits * (1 - skip)[:, :, None], axis=1).astype(jnp.int32)


def aggregate(embed, cached, fresh_flags, tiles, tile_pos):
    feat_width = embed.shape[1]
    new_blocks = embed.reshape(NB, 2, TS, feat_width)
    old_blocks = cached.reshape(NB, 2, TS, feat_width)
    block_ids = jnp.arange(NB, dtype=jnp.int32)

    def per_block(operands):
        block_index, tile_row, pos_row = operands
        use_new = (fresh_flags == 1) | (block_ids == block_index)
        source = jnp.where(use_new[:, None, None, None], new_blocks, old_blocks)
        halves = jnp.where((pos_row[:, 1] == 0)[:, None, None], source[:, 0], source[:, 1])
        products = jnp.einsum("kab,kbf->kaf", tile_row.astype(jnp.float32), halves.astype(jnp.float32))
        upper = (pos_row[:, 0] == 0)[:, None, None]
        upper_sum = jnp.sum(jnp.where(upper, products, jnp.float32(0.0)), axis=0)
        lower_sum = jnp.sum(jnp.where(upper, jnp.float32(0.0), products), axis=0)
        return jnp.concatenate([upper_sum, lower_sum], axis=0)

    summed = lax.map(per_block, (block_ids, tiles, tile_pos))
    return summed.reshape(NB * V_DEV, feat_width)


def reference(features, cache_in, cache_hidden, tiles, tile_pos, order, skip, w_first, w_second):
    fresh_flags = refreshed_flags(order, skip)
    first_agg = aggregate(features, cache_in, fresh_flags[0], tiles, tile_pos).astype(jnp.bfloat16)
    hidden = jnp.maximum(jnp.dot(first_agg, w_first, preferred_element_type=jnp.float32), 0.0).astype(jnp.bfloat16)
    second_agg = aggregate(hidden, cache_hidden, fresh_flags[1], tiles, tile_pos).astype(jnp.bfloat16)
    output = jnp.dot(second_agg, w_second, preferred_element_type=jnp.float32).astype(jnp.bfloat16)
    input_change = features.astype(jnp.float32) - cache_in.astype(jnp.float32)
    hidden_change = hidden.astype(jnp.float32) - cache_hidden.astype(jnp.float32)
    drift = jnp.stack([jnp.sum(input_change * input_change) / (NB * V_DEV * F),
                       jnp.sum(hidden_change * hidden_change) / (NB * V_DEV * HID)])
    return output, drift
```

```python
import jax
import jax.numpy as jnp
from jax import lax
from jax.experimental import pallas as pl
from jax.experimental.pallas import tpu as pltpu
from jax.sharding import Mesh
from jax.sharding import PartitionSpec as P

AXES = ("ylo", "x", "core", "z", "yhi")
NB = 128
ROWS = 512
TS = 256
W = 128
DEPTH = 8
PIECES = 12
AX = ((1, 2, 0), (2, 0, 1))


def coords(i):
    return [(i // 16) % 4, (i % 2) * 2 + i // 64, (i // 2) % 4, (i // 8) % 2]


def block_id(x, y, z, core):
    return (y % 2) * 64 + x * 16 + core * 8 + z * 2 + y // 2


def stage_perm(stage, shift):
    pairs = []
    for i in range(NB):
        c = coords(i)
        a = AX[c[3]][stage]
        c[a] = (c[a] + shift) % 4
        pairs.append((i, block_id(*c)))
    return pairs


PERM = {(s, k): stage_perm(s, k) for s in range(3) for k in (1, 2, 3)}
SWAP = [(i, i ^ 8) for i in range(NB)]


def shift(value, stage, k):
    return lax.ppermute(value, AXES, PERM[(stage, k)])


def swap(value):
    return lax.ppermute(value, AXES, SWAP)


def gather(block):
    s1 = block[None]
    s4 = jnp.concatenate([s1] + [shift(s1, 0, k) for k in (1, 2, 3)], 0)
    s16 = jnp.concatenate([s4] + [shift(s4, 1, k) for k in (1, 2, 3)], 0)
    lo, hi = s16[:8], s16[8:]
    a1 = shift(lo, 2, 1)
    b3 = shift(hi, 2, 3)
    b1 = shift(hi, 2, 1)
    a3 = shift(lo, 2, 3)
    f1 = shift(a1, 2, 1)
    f3 = shift(b3, 2, 3)
    mine = [a1, b3, b1, a3, f1, f3]
    theirs = [swap(p) for p in mine]
    return in_vmem(s16), in_vmem(swap(s16)), [in_vmem(p) for p in mine + theirs]


def item_blocks():
    k1, k2, k3, other = [], [], [], []

    def add(slots, third, o):
        for s in slots:
            k1.append(s % 4)
            k2.append(s // 4)
            k3.append(third)
            other.append(o)

    for o in (0, 1):
        add(range(16), 0, o)
    for o in (0, 1):
        for slots, third in ((0, 1), (8, 3), (8, 1), (0, 3), (0, 2), (8, 2)):
            add(range(slots, slots + 8), third, o)
    k1, k2, k3, other = (jnp.array(v, jnp.int32) for v in (k1, k2, k3, other))
    x = lax.axis_index("x")
    y = lax.axis_index("yhi") * 2 + lax.axis_index("ylo")
    z = lax.axis_index("z")
    core = lax.axis_index("core") ^ other
    zero = core == 0
    bx = (x - jnp.where(zero, k3, k2)) & 3
    by = (y - jnp.where(zero, k1, k3)) & 3
    bz = (z - jnp.where(zero, k2, k1)) & 3
    return (by & 1) * 64 + bx * 16 + core * 8 + bz * 2 + (by >> 1)


def fill(first, total, start):
    for d in range(DEPTH):
        @pl.when(first + d < total)
        def _(d=d):
            start(first + d, d)


def run(first, last, total, start, consume):
    def body(t, c):
        slot = t & (DEPTH - 1)
        consume(t, slot)

        @pl.when(t + DEPTH < total)
        def _():
            start(t + DEPTH, slot)

        return c

    lax.fori_loop(first, last, body, 0)


def half_of(ref, code):
    return ref[code >> 16, pl.ds(((code >> 1) & 1) * TS, TS), :]


def accumulate(code, acc, tile, source):
    acc[pl.ds((code & 1) * TS, TS), :] += jnp.dot(
        tile, source, preferred_element_type=jnp.float32
    )


def early_kernel(
    order, skip, pos, jtab, own, tiles, cached, s16, p16, block,
    acc, flist, foff, drift,
    clist, slist, flags, tbuf, sbuf, own_buf, tsem, ssem, osem,
):
    me = own[0]
    own_copy = pltpu.make_async_copy(cached.at[me], own_buf, osem)
    own_copy.start()

    def set_flag(r, c):
        flags[order[r]] = 1 - skip[r]
        return c

    lax.fori_loop(0, NB, set_flag, 0)
    flags[me] = 1

    def code_of(t, slot):
        j = jtab[t]
        return flags[j], (slot << 16) | (j << 4) | (pos[2 * j + 1] << 1) | pos[2 * j]

    def build(t, c, slot_mask, fresh_list):
        nc, nl = c
        fresh, code = code_of(t, t & slot_mask)
        clist[nc] = code
        fresh_list[nl] = code
        return nc + 1 - fresh, nl + fresh

    nc, n_own = lax.fori_loop(0, 16, lambda t, c: build(t, c, 15, slist), (0, 0))
    nc, n_near = lax.fori_loop(16, 32, lambda t, c: build(t, c, 15, slist), (nc, n_own))
    nl = 0
    for p in range(PIECES):
        foff[p] = nl
        nc, nl = lax.fori_loop(
            32 + 8 * p, 40 + 8 * p, lambda t, c: build(t, c, 7, flist), (nc, nl)
        )
    foff[PIECES] = nl
    acc[...] = jnp.zeros_like(acc)

    def tile_copy(code, slot):
        return pltpu.make_async_copy(
            tiles.at[(code >> 4) & 127], tbuf.at[slot], tsem.at[slot]
        )

    def source_copy(code, slot):
        return pltpu.make_async_copy(
            cached.at[(code >> 4) & 127, pl.ds(((code >> 1) & 1) * TS, TS), :],
            sbuf.at[slot],
            ssem.at[slot],
        )

    def start(t, slot):
        code = clist[t]
        tile_copy(code, slot).start()
        source_copy(code, slot).start()

    def consume(t, slot):
        code = clist[t]
        tile_copy(code, slot).wait()
        source_copy(code, slot).wait()
        accumulate(code, acc, tbuf[slot], sbuf[slot])

    fill(0, nc, start)
    run(0, nc, nc, start, consume)

    def start_near(t, slot):
        tile_copy(slist[t], slot).start()

    def near(ref):
        def consume_near(t, slot):
            code = slist[t]
            tile_copy(code, slot).wait()
            accumulate(code, acc, tbuf[slot], half_of(ref, code))

        return consume_near

    fill(0, n_near, start_near)
    run(0, n_own, n_near, start_near, near(s16))
    run(n_own, n_near, n_near, start_near, near(p16))
    own_copy.wait()
    diff = block[0:ROWS, :].astype(jnp.float32) - own_buf[...].astype(jnp.float32)
    drift[...] = jnp.broadcast_to(jnp.sum(diff * diff, axis=0, keepdims=True), (8, W))


def late_ring(flist, foff, acc_in, tiles, pieces, acc, tbuf, tsem):
    acc[...] = acc_in[...]
    total = foff[PIECES]

    def tile_copy(code, slot):
        return pltpu.make_async_copy(
            tiles.at[(code >> 4) & 127], tbuf.at[slot], tsem.at[slot]
        )

    def start(t, slot):
        tile_copy(flist[t], slot).start()

    fill(0, total, start)
    for p, ref in enumerate(pieces):
        def consume(t, slot, ref=ref):
            code = flist[t]
            tile_copy(code, slot).wait()
            accumulate(code, acc, tbuf[slot], half_of(ref, code))

        run(foff[p], foff[p + 1], total, start, consume)


def split3(row):
    hi = row.astype(jnp.bfloat16).astype(jnp.float32)
    mid = (row - hi).astype(jnp.bfloat16).astype(jnp.float32)
    return hi, mid, row - hi - mid


def late_first_kernel(
    flist, foff, own, acc_in, drift_in, weight, tiles, cached, *rest
):
    pieces = rest[:PIECES]
    payload, acc, tbuf, own_buf, tsem, osem = rest[PIECES:]
    own_copy = pltpu.make_async_copy(cached.at[own[0]], own_buf, osem)
    own_copy.start()
    late_ring(flist, foff, acc_in, tiles, pieces, acc, tbuf, tsem)
    hidden = jnp.maximum(
        jnp.dot(
            acc[...].astype(jnp.bfloat16), weight[...], preferred_element_type=jnp.float32
        ),
        0.0,
    ).astype(jnp.bfloat16)
    payload[0:ROWS, :] = hidden
    own_copy.wait()
    diff = hidden.astype(jnp.float32) - own_buf[...].astype(jnp.float32)
    second = jnp.sum(diff * diff, axis=0, keepdims=True)
    row = lax.broadcasted_iota(jnp.int32, (16, W), 0)
    extra = jnp.zeros((16, W), jnp.float32)
    for k, part in enumerate(split3(drift_in[0:1, :]) + split3(second)):
        extra = jnp.where(row == k, jnp.broadcast_to(part, (16, W)), extra)
    payload[ROWS:, :] = extra.astype(jnp.bfloat16)


def late_second_kernel(
    flist, foff, jtab, acc_in, weight, tiles, s16, p16, *rest
):
    pieces = rest[:PIECES]
    output, drift, acc, tbuf, ext, tsem = rest[PIECES:]
    late_ring(flist, foff, acc_in, tiles, pieces, acc, tbuf, tsem)
    for base, ref, n in [(0, s16, 16), (16, p16, 16)] + [
        (32 + 8 * k, ref, 8) for k, ref in enumerate(pieces)
    ]:
        for s in range(n):
            ext[jtab[base + s]] = ref[s, ROWS:, :]
    output[...] = jnp.dot(
        acc[...].astype(jnp.bfloat16), weight[...], preferred_element_type=jnp.float32
    ).astype(jnp.bfloat16)
    total = jnp.sum(ext[...].astype(jnp.float32), axis=0)
    cells = 1.0 / (NB * ROWS * W)
    drift[0] = jnp.sum(total[0:3, :]) * cells
    drift[1] = jnp.sum(total[3:6, :]) * cells


SMEM = pl.BlockSpec(memory_space=pltpu.SMEM)
VMEM = pl.BlockSpec(memory_space=pltpu.VMEM)
HBM = pl.BlockSpec(memory_space=pltpu.HBM)


TILE_RING = pltpu.VMEM((DEPTH, TS, TS), jnp.bfloat16)
RING_SEMS = pltpu.SemaphoreType.DMA((DEPTH,))
PARAMS = pltpu.CompilerParams(vmem_limit_bytes=24 * 1024 * 1024)


def cost(items):
    return pl.CostEstimate(
        flops=items * 2 * TS * TS * W, transcendentals=0, bytes_accessed=items * 196608
    )


def early(order, skip, pos, jtab, own, tiles, cached, s16, p16, block, name):
    return pl.pallas_call(
        early_kernel,
        out_shape=(
            jax.ShapeDtypeStruct((ROWS, W), jnp.float32),
            jax.ShapeDtypeStruct((NB,), jnp.int32),
            jax.ShapeDtypeStruct((16,), jnp.int32),
            jax.ShapeDtypeStruct((8, W), jnp.float32),
        ),
        in_specs=[SMEM] * 5 + [HBM] * 2 + [VMEM] * 3,
        out_specs=(VMEM, SMEM, SMEM, VMEM),
        scratch_shapes=[
            pltpu.SMEM((NB + 8,), jnp.int32),
            pltpu.SMEM((64,), jnp.int32),
            pltpu.SMEM((NB,), jnp.int32),
            TILE_RING,
            pltpu.VMEM((DEPTH, TS, W), jnp.bfloat16),
            pltpu.VMEM((ROWS, W), jnp.bfloat16),
            RING_SEMS,
            RING_SEMS,
            pltpu.SemaphoreType.DMA,
        ],
        compiler_params=PARAMS,
        cost_estimate=cost(80),
        name=name,
    )(order, skip, pos, jtab, own, tiles, cached, s16, p16, block)


def late_first(flist, foff, own, acc, drift, weight, tiles, cached, pieces):
    return pl.pallas_call(
        late_first_kernel,
        out_shape=jax.ShapeDtypeStruct((ROWS + 16, W), jnp.bfloat16),
        in_specs=[SMEM] * 3 + [VMEM] * 3 + [HBM] * 2 + [VMEM] * PIECES,
        out_specs=VMEM,
        scratch_shapes=[
            pltpu.VMEM((ROWS, W), jnp.float32),
            TILE_RING,
            pltpu.VMEM((ROWS, W), jnp.bfloat16),
            RING_SEMS,
            pltpu.SemaphoreType.DMA,
        ],
        compiler_params=PARAMS,
        cost_estimate=cost(48),
        name="late_first",
    )(flist, foff, own, acc, drift, weight, tiles, cached, *pieces)


def late_second(flist, foff, jtab, acc, weight, tiles, s16, p16, pieces):
    return pl.pallas_call(
        late_second_kernel,
        out_shape=(
            jax.ShapeDtypeStruct((ROWS, W), jnp.bfloat16),
            jax.ShapeDtypeStruct((2,), jnp.float32),
        ),
        in_specs=[SMEM] * 3 + [VMEM] * 2 + [HBM] + [VMEM] * (2 + PIECES),
        out_specs=(VMEM, SMEM),
        scratch_shapes=[
            pltpu.VMEM((ROWS, W), jnp.float32),
            TILE_RING,
            pltpu.VMEM((NB, 16, W), jnp.bfloat16),
            RING_SEMS,
        ],
        compiler_params=PARAMS,
        cost_estimate=cost(48),
        name="late_second",
    )(flist, foff, jtab, acc, weight, tiles, s16, p16, *pieces)


def in_hbm(value):
    return pltpu.with_memory_space_constraint(value, pltpu.HBM)


def in_vmem(value):
    return pltpu.with_memory_space_constraint(value, pltpu.VMEM)


def on_device(features, cache_in, cache_hidden, tiles, tile_pos, order, skip, w_first, w_second):
    tiles = in_hbm(tiles[0])
    pos = tile_pos[0].reshape(2 * NB)
    own = lax.axis_index(AXES)[None].astype(jnp.int32)
    jtab = item_blocks()
    cache_in = in_hbm(cache_in.reshape(NB, ROWS, W))
    cache_hidden = in_hbm(cache_hidden.reshape(NB, ROWS, W))

    s16, p16, pieces = gather(features)
    acc, flist, foff, drift_in = early(
        order[0], skip[0], pos, jtab, own, tiles, cache_in, s16, p16, features, "early_first"
    )
    payload = late_first(flist, foff, own, acc, drift_in, w_first, tiles, cache_hidden, pieces)

    s16, p16, pieces = gather(payload)
    acc, flist, foff, _ = early(
        order[1], skip[1], pos, jtab, own, tiles, cache_hidden, s16, p16, payload, "early_second"
    )
    return late_second(flist, foff, jtab, acc, w_second, tiles, s16, p16, pieces)


def solution(mesh):
    split = Mesh(mesh.devices.reshape(2, 4, 2, 4, 2), AXES)
    both = AXES
    in_specs = (
        P(both, None),
        P(),
        P(),
        P(both, None, None, None),
        P(both, None, None),
        P(),
        P(),
        P(),
        P(),
    )
    out_specs = (P(both, None), P())
    return jax.shard_map(
        on_device, mesh=split, in_specs=in_specs, out_specs=out_specs, check_vma=False
    )
```

```python
import jax
import jax.numpy as jnp
from jax import lax
from jax.experimental import pallas as pl
from jax.experimental.pallas import tpu as pltpu
from jax.sharding import Mesh
from jax.sharding import PartitionSpec as P


AXES = ("ylo", "x", "core", "z", "yhi")
NB = 128
ROWS = 512
TS = 256
W = 128
DEPTH = 8
UNROLL = 4
MID = 8
LATE = 4
AX = ((1, 2, 0), (2, 0, 1))


def coords(i):
    return [(i // 16) % 4, (i % 2) * 2 + i // 64, (i // 2) % 4, (i // 8) % 2]


def block_id(x, y, z, core):
    return (y % 2) * 64 + x * 16 + core * 8 + z * 2 + y // 2


def stage_perm(stage, shift):
    pairs = []
    for i in range(NB):
        c = coords(i)
        a = AX[c[3]][stage]
        c[a] = (c[a] + shift) % 4
        pairs.append((i, block_id(*c)))
    return pairs


PERM = {(s, k): stage_perm(s, k) for s in range(3) for k in (1, 2, 3)}
SWAP = [(i, i ^ 8) for i in range(NB)]


def shift(value, stage, k):
    return lax.ppermute(value, AXES, PERM[(stage, k)])


def swap(value):
    return lax.ppermute(value, AXES, SWAP)


def gather(block):
    s1 = block[None]
    s4 = jnp.concatenate([s1] + [shift(s1, 0, k) for k in (1, 2, 3)], 0)
    s16 = jnp.concatenate([s4] + [shift(s4, 1, k) for k in (1, 2, 3)], 0)
    lo, hi = s16[:8], s16[8:]
    a1 = shift(lo, 2, 1)
    b3 = shift(hi, 2, 3)
    b1 = shift(hi, 2, 1)
    a3 = shift(lo, 2, 3)
    f1 = shift(a1, 2, 1)
    f3 = shift(b3, 2, 3)
    near = [s16, swap(s16)]
    mid = [a1, b3, b1, a3]
    mid += [swap(p) for p in mid]
    late = [f1, f3]
    late += [swap(p) for p in late]
    return near, mid, late


def item_blocks():
    k1, k2, k3, other = [], [], [], []

    def add(slots, third, o):
        for s in slots:
            k1.append(s % 4)
            k2.append(s // 4)
            k3.append(third)
            other.append(o)

    for o in (0, 1):
        add(range(16), 0, o)
    for group in (((0, 1), (8, 3), (8, 1), (0, 3)), ((0, 2), (8, 2))):
        for o in (0, 1):
            for slots, third in group:
                add(range(slots, slots + 8), third, o)
    k1, k2, k3, other = (jnp.array(v, jnp.int32) for v in (k1, k2, k3, other))
    x = lax.axis_index("x")
    y = lax.axis_index("yhi") * 2 + lax.axis_index("ylo")
    z = lax.axis_index("z")
    core = lax.axis_index("core") ^ other
    zero = core == 0
    bx = (x - jnp.where(zero, k3, k2)) & 3
    by = (y - jnp.where(zero, k1, k3)) & 3
    bz = (z - jnp.where(zero, k2, k1)) & 3
    return (by & 1) * 64 + bx * 16 + core * 8 + bz * 2 + (by >> 1)


def groups_of(n):
    return (n + (UNROLL - 1)) // UNROLL


def pad(ref, n):
    for u in range(UNROLL - 1):
        ref[n + u] = 2


def tile_copy(tiles, tbuf, tsem, code, slot):
    return pltpu.make_async_copy(tiles.at[(code >> 4) & 127], tbuf.at[slot], tsem.at[slot])


def run(n, start, wait, source, codes, accs, tbuf):
    total = groups_of(n) * UNROLL
    for d in range(DEPTH):
        @pl.when(d < total)
        def _(d=d):
            start(d, d)

    def body(g, c):
        first = g * UNROLL
        slot0 = (g & (DEPTH // UNROLL - 1)) * UNROLL
        for u in range(UNROLL):
            wait(first + u, slot0 + u)
        for u in range(UNROLL):
            up = (codes[first + u] & 3) * TS
            accs[u, pl.ds(up, TS), :] += jnp.dot(
                tbuf[slot0 + u],
                source(first + u, slot0 + u),
                preferred_element_type=jnp.float32,
            )
        for u in range(UNROLL):
            @pl.when(first + u + DEPTH < total)
            def _(u=u):
                start(first + u + DEPTH, slot0 + u)
        return c

    lax.fori_loop(0, groups_of(n), body, 0)


def run_staged(n, codes, accs, tiles, tbuf, tsem, stage):
    run(
        n,
        lambda t, slot: tile_copy(tiles, tbuf, tsem, codes[t], slot).start(),
        lambda t, slot: tile_copy(tiles, tbuf, tsem, codes[t], slot).wait(),
        lambda t, slot: stage[t],
        codes,
        accs,
        tbuf,
    )


def fill_stage(codes, first, last, ref, stage):
    def body(t, c):
        code = codes[t]
        stage[t] = ref[code >> 16, pl.ds(((code >> 2) & 1) * TS, TS), :]
        return c

    lax.fori_loop(first, last, body, 0)


def total_of(accs):
    total = accs[0, 0:ROWS, :]
    for u in range(1, UNROLL):
        total = total + accs[u, 0:ROWS, :]
    return total


def early_kernel(
    order, skip, pos, jtab, own, tiles, cached, s16, p16, block,
    acc, mlist, moff, llist, loff, drift,
    clist, slist, flags, accs, tbuf, sbuf, stage, own_buf, tsem, ssem, osem,
):
    me = own[0]
    own_copy = pltpu.make_async_copy(cached.at[me], own_buf, osem)
    own_copy.start()

    def set_flag(r, c):
        flags[order[r]] = 1 - skip[r]
        return c

    lax.fori_loop(0, NB, set_flag, 0)
    flags[me] = 1

    def split(first, last, nc, nl, slots, fresh_list):
        def build(t, c):
            nc, nl = c
            j = jtab[t]
            fresh = flags[j]
            code = ((t & (slots - 1)) << 16) | (j << 4) | (pos[2 * j + 1] << 2) | pos[2 * j]
            clist[nc] = code
            fresh_list[nl] = code
            return nc + 1 - fresh, nl + fresh

        return lax.fori_loop(first, last, build, (nc, nl))

    nc, n_own = split(0, 16, 0, 0, 16, slist)
    nc, n_near = split(16, 32, nc, n_own, 16, slist)
    base = 32
    for pieces, fresh_list, off in ((MID, mlist, moff), (LATE, llist, loff)):
        nl = 0
        for p in range(pieces):
            off[p] = nl
            nc, nl = split(base, base + 8, nc, nl, 8, fresh_list)
            base += 8
        off[pieces] = nl
        pad(fresh_list, nl)
    pad(clist, nc)
    pad(slist, n_near)
    accs[...] = jnp.zeros_like(accs)

    def source_copy(t, slot):
        code = clist[t]
        return pltpu.make_async_copy(
            cached.at[(code >> 4) & 127, pl.ds(((code >> 2) & 1) * TS, TS), :],
            sbuf.at[slot],
            ssem.at[slot],
        )

    def start(t, slot):
        tile_copy(tiles, tbuf, tsem, clist[t], slot).start()
        source_copy(t, slot).start()

    def wait(t, slot):
        tile_copy(tiles, tbuf, tsem, clist[t], slot).wait()
        source_copy(t, slot).wait()

    run(nc, start, wait, lambda t, slot: sbuf[slot], clist, accs, tbuf)
    fill_stage(slist, 0, n_own, s16, stage)
    fill_stage(slist, n_own, n_near, p16, stage)
    run_staged(n_near, slist, accs, tiles, tbuf, tsem, stage)
    acc[...] = total_of(accs)
    own_copy.wait()
    diff = block[0:ROWS, :].astype(jnp.float32) - own_buf[...].astype(jnp.float32)
    drift[...] = jnp.broadcast_to(jnp.sum(diff * diff, axis=0, keepdims=True), (8, W))


def add_pieces(codes, off, tiles, pieces, accs, tbuf, stage, tsem):
    accs[...] = jnp.zeros_like(accs)
    for p, ref in enumerate(pieces):
        fill_stage(codes, off[p], off[p + 1], ref, stage)
    run_staged(off[len(pieces)], codes, accs, tiles, tbuf, tsem, stage)
    return total_of(accs)


def mid_kernel(codes, off, acc_in, tiles, *rest):
    pieces = rest[:MID]
    acc, accs, tbuf, stage, tsem = rest[MID:]
    acc[...] = acc_in[...] + add_pieces(codes, off, tiles, pieces, accs, tbuf, stage, tsem)


def split3(row):
    hi = row.astype(jnp.bfloat16).astype(jnp.float32)
    mid = (row - hi).astype(jnp.bfloat16).astype(jnp.float32)
    return hi, mid, row - hi - mid


def late_first_kernel(
    codes, off, own, acc_in, drift_in, weight, tiles, cached, *rest
):
    pieces = rest[:LATE]
    payload, accs, tbuf, stage, own_buf, tsem, osem = rest[LATE:]
    own_copy = pltpu.make_async_copy(cached.at[own[0]], own_buf, osem)
    own_copy.start()
    total = acc_in[...] + add_pieces(codes, off, tiles, pieces, accs, tbuf, stage, tsem)
    hidden = jnp.maximum(
        jnp.dot(
            total.astype(jnp.bfloat16), weight[...], preferred_element_type=jnp.float32
        ),
        0.0,
    ).astype(jnp.bfloat16)
    payload[0:ROWS, :] = hidden
    own_copy.wait()
    diff = hidden.astype(jnp.float32) - own_buf[...].astype(jnp.float32)
    second = jnp.sum(diff * diff, axis=0, keepdims=True)
    row = lax.broadcasted_iota(jnp.int32, (16, W), 0)
    extra = jnp.zeros((16, W), jnp.float32)
    for k, part in enumerate(split3(drift_in[0:1, :]) + split3(second)):
        extra = jnp.where(row == k, jnp.broadcast_to(part, (16, W)), extra)
    payload[ROWS:, :] = extra.astype(jnp.bfloat16)


def late_second_kernel(codes, off, jtab, acc_in, weight, tiles, *rest):
    pieces = rest[: 2 + MID + LATE]
    output, drift, accs, tbuf, stage, ext, tsem = rest[2 + MID + LATE :]
    total = acc_in[...] + add_pieces(
        codes, off, tiles, pieces[2 + MID :], accs, tbuf, stage, tsem
    )
    output[...] = jnp.dot(
        total.astype(jnp.bfloat16), weight[...], preferred_element_type=jnp.float32
    ).astype(jnp.bfloat16)
    base = 0
    for ref in pieces:
        for s in range(ref.shape[0]):
            ext[jtab[base + s]] = ref[s, ROWS:, :]
        base += ref.shape[0]
    total = jnp.sum(ext[...].astype(jnp.float32), axis=0)
    cells = 1.0 / (NB * ROWS * W)
    drift[0] = jnp.sum(total[0:3, :]) * cells
    drift[1] = jnp.sum(total[3:6, :]) * cells


SMEM = pl.BlockSpec(memory_space=pltpu.SMEM)
VMEM = pl.BlockSpec(memory_space=pltpu.VMEM)
HBM = pl.BlockSpec(memory_space=pltpu.HBM)


ACCS = pltpu.VMEM((UNROLL, 3 * TS, W), jnp.float32)
TILE_RING = pltpu.VMEM((DEPTH, TS, TS), jnp.bfloat16)
RING_SEMS = pltpu.SemaphoreType.DMA((DEPTH,))
BLOCK = pltpu.VMEM((ROWS, W), jnp.bfloat16)


def stage_of(items):
    return pltpu.VMEM((items + UNROLL, TS, W), jnp.bfloat16)


def params(mib):
    return pltpu.CompilerParams(vmem_limit_bytes=mib * 1024 * 1024)


def cost(items):
    return pl.CostEstimate(
        flops=items * 2 * TS * TS * W, transcendentals=0, bytes_accessed=items * 196608
    )


def codes_shape(items):
    return jax.ShapeDtypeStruct((items + 16,), jnp.int32)


def early(order, skip, pos, jtab, own, tiles, cached, near, block):
    return pl.pallas_call(
        early_kernel,
        out_shape=(
            jax.ShapeDtypeStruct((ROWS, W), jnp.float32),
            codes_shape(8 * MID),
            jax.ShapeDtypeStruct((16,), jnp.int32),
            codes_shape(8 * LATE),
            jax.ShapeDtypeStruct((16,), jnp.int32),
            jax.ShapeDtypeStruct((8, W), jnp.float32),
        ),
        in_specs=[SMEM] * 5 + [HBM] * 2 + [VMEM] * 3,
        out_specs=(VMEM, SMEM, SMEM, SMEM, SMEM, VMEM),
        scratch_shapes=[
            pltpu.SMEM((NB + 8,), jnp.int32),
            pltpu.SMEM((64,), jnp.int32),
            pltpu.SMEM((NB,), jnp.int32),
            ACCS,
            TILE_RING,
            pltpu.VMEM((DEPTH, TS, W), jnp.bfloat16),
            stage_of(32),
            BLOCK,
            RING_SEMS,
            RING_SEMS,
            pltpu.SemaphoreType.DMA,
        ],
        compiler_params=params(16),
        cost_estimate=cost(80),
        name="early_sum",
    )(order, skip, pos, jtab, own, tiles, cached, *near, block)


def mid_sum(codes, off, acc, tiles, pieces):
    return pl.pallas_call(
        mid_kernel,
        out_shape=jax.ShapeDtypeStruct((ROWS, W), jnp.float32),
        in_specs=[SMEM] * 2 + [VMEM] + [HBM] + [VMEM] * MID,
        out_specs=VMEM,
        scratch_shapes=[ACCS, TILE_RING, stage_of(8 * MID), RING_SEMS],
        compiler_params=params(20),
        cost_estimate=cost(32),
        name="mid_sum",
    )(codes, off, acc, tiles, *pieces)


def late_first(codes, off, own, acc, drift, weight, tiles, cached, pieces):
    return pl.pallas_call(
        late_first_kernel,
        out_shape=jax.ShapeDtypeStruct((ROWS + 16, W), jnp.bfloat16),
        in_specs=[SMEM] * 3 + [VMEM] * 3 + [HBM] * 2 + [VMEM] * LATE,
        out_specs=VMEM,
        scratch_shapes=[
            ACCS,
            TILE_RING,
            stage_of(8 * LATE),
            BLOCK,
            RING_SEMS,
            pltpu.SemaphoreType.DMA,
        ],
        compiler_params=params(16),
        cost_estimate=cost(16),
        name="late_first",
    )(codes, off, own, acc, drift, weight, tiles, cached, *pieces)


def late_second(codes, off, jtab, acc, weight, tiles, pieces):
    return pl.pallas_call(
        late_second_kernel,
        out_shape=(
            jax.ShapeDtypeStruct((ROWS, W), jnp.bfloat16),
            jax.ShapeDtypeStruct((2,), jnp.float32),
        ),
        in_specs=[SMEM] * 3 + [VMEM] * 2 + [HBM] + [VMEM] * len(pieces),
        out_specs=(VMEM, SMEM),
        scratch_shapes=[
            ACCS,
            TILE_RING,
            stage_of(8 * LATE),
            pltpu.VMEM((NB, 16, W), jnp.bfloat16),
            RING_SEMS,
        ],
        compiler_params=params(20),
        cost_estimate=cost(16),
        name="late_second",
    )(codes, off, jtab, acc, weight, tiles, *pieces)


def in_hbm(value):
    return pltpu.with_memory_space_constraint(value, pltpu.HBM)


def on_device(features, cache_in, cache_hidden, tiles, tile_pos, order, skip, w_first, w_second):
    tiles = in_hbm(tiles[0])
    pos = tile_pos[0].reshape(2 * NB)
    own = lax.axis_index(AXES)[None].astype(jnp.int32)
    jtab = item_blocks()
    cache_in = in_hbm(cache_in.reshape(NB, ROWS, W))
    cache_hidden = in_hbm(cache_hidden.reshape(NB, ROWS, W))

    near, mid, late = gather(features)
    acc, mlist, moff, llist, loff, drift_in = early(
        order[0], skip[0], pos, jtab, own, tiles, cache_in, near, features
    )
    acc = mid_sum(mlist, moff, acc, tiles, mid)
    payload = late_first(
        llist, loff, own, acc, drift_in, w_first, tiles, cache_hidden, late
    )

    near, mid, late = gather(payload)
    acc, mlist, moff, llist, loff, _ = early(
        order[1], skip[1], pos, jtab, own, tiles, cache_hidden, near, payload
    )
    acc = mid_sum(mlist, moff, acc, tiles, mid)
    return late_second(llist, loff, jtab, acc, w_second, tiles, near + mid + late)


def solution(mesh):
    split = Mesh(mesh.devices.reshape(2, 4, 2, 4, 2), AXES)
    both = AXES
    in_specs = (
        P(both, None),
        P(),
        P(),
        P(both, None, None, None),
        P(both, None, None),
        P(),
        P(),
        P(),
        P(),
    )
    out_specs = (P(both, None), P())
    return jax.shard_map(
        on_device, mesh=split, in_specs=in_specs, out_specs=out_specs, check_vma=False
    )
```

```python
import functools

import jax
import jax.numpy as jnp
from jax import lax
from jax.experimental import pallas as pl
from jax.experimental.pallas import tpu as pltpu
from jax.sharding import Mesh
from jax.sharding import PartitionSpec as P


AXES = ("ylo", "x", "core", "z", "yhi")
NB = 128
ROWS = 512
TS = 256
W = 128
UNROLL = 4
AX = ((1, 2, 0), (0, 2, 1))
QA = [(k, 0) for k in range(4)]
QB = [(k, 1) for k in range(4)] + [(k, 3) for k in range(4)]
QC = [(k, 2) for k in range(4)]
GROUPS = (
    ((QA, 0), (QA, 1), (QA, 3), (QA, 2), (QB, 0), (QC, 0)),
    ((QB, 1), (QB, 3)),
    ((QC, 1), (QC, 3), (QB, 2), (QC, 2)),
)


def sizes(group):
    return [len(q) for q, _ in GROUPS[group]]


def coords(i):
    return [(i // 16) % 4, (i % 2) * 2 + i // 64, (i // 2) % 4, (i // 8) % 2]


def block_id(x, y, z, core):
    return (y % 2) * 64 + x * 16 + core * 8 + z * 2 + y // 2


def stage_perm(stage, shift):
    pairs = []
    for i in range(NB):
        c = coords(i)
        a = AX[c[3]][stage]
        c[a] = (c[a] + shift) % 4
        pairs.append((i, block_id(*c)))
    return pairs


PERM = {(s, k): stage_perm(s, k) for s in range(3) for k in (1, 2, 3)}
SWAP = [(i, i ^ 8) for i in range(NB)]


def shift(value, stage, k):
    return lax.ppermute(value, AXES, PERM[(stage, k)])


def swap(value):
    return lax.ppermute(value, AXES, SWAP)


def gather(block):
    s1 = block[None]
    qa = jnp.concatenate([s1] + [shift(s1, 0, k) for k in (1, 2, 3)], 0)
    q1, q3, q2 = (shift(qa, 1, k) for k in (1, 3, 2))
    ap = shift(qa, 2, 1)
    am = shift(qa, 2, 3)
    fa = shift(ap, 2, 1)
    qb = jnp.concatenate([q1, q3], 0)
    bp = shift(qb, 2, 1)
    bm = shift(qb, 2, 3)
    fb = shift(bm, 2, 3)
    cp = shift(q2, 2, 1)
    cm = shift(q2, 2, 3)
    fc = shift(cp, 2, 1)
    return [qa, ap, am, fa, qb, q2], [bp, bm], [cp, cm, fb, fc]


def item_blocks():
    k1, k2, k3 = [], [], []
    for group in GROUPS:
        for slots, third in group:
            for first, second in slots:
                k1.append(first)
                k2.append(second)
                k3.append(third)
    k1, k2, k3 = (jnp.array(v, jnp.int32) for v in (k1, k2, k3))
    core = lax.axis_index("core")
    y = lax.axis_index("yhi") * 2 + lax.axis_index("ylo")
    zero = core == 0
    bx = (lax.axis_index("x") - jnp.where(zero, k3, k1)) & 3
    by = (y - jnp.where(zero, k1, k3)) & 3
    bz = (lax.axis_index("z") - k2) & 3
    return (by & 1) * 64 + bx * 16 + core * 8 + bz * 2 + (by >> 1)


PADDING = 4


def groups_of(n):
    return (n + (UNROLL - 1)) // UNROLL


def pad(ref, n):
    for u in range(UNROLL - 1):
        ref[n + u] = PADDING


def half_rows(code):
    return pl.ds(((code >> 3) & 1) * TS, TS)


def start_tile(tiles, other, tbuf, tsem, code, slot):
    block = (code >> 4) & 127
    theirs = (code >> 1) & 1

    @pl.when(theirs == 0)
    def _():
        pltpu.make_async_copy(tiles.at[block], tbuf.at[slot], tsem.at[slot]).start()

    @pl.when(theirs == 1)
    def _():
        pltpu.make_async_copy(other.at[block], tbuf.at[slot], tsem.at[slot]).start()


def wait_tile(tiles, tbuf, tsem, slot):
    pltpu.make_async_copy(tiles.at[0], tbuf.at[slot], tsem.at[slot]).wait()


def run(n, start, wait, source, codes, accs, tbuf):
    depth = tbuf.shape[0]
    total = groups_of(n) * UNROLL

    def prime(t, c):
        start(t, t)
        return c

    lax.fori_loop(0, jnp.minimum(total, depth), prime, 0)

    def body(g, c):
        first = g * UNROLL
        slot0 = first & (depth - 1)
        for u in range(UNROLL):
            wait(first + u, slot0 + u)
        for u in range(UNROLL):
            rows = pl.ds((codes[first + u] & 7) * TS, TS)
            accs[u, rows, :] += jnp.dot(
                tbuf[slot0 + u],
                source(first + u, slot0 + u),
                preferred_element_type=jnp.float32,
            )

        @pl.when(first + depth < total)
        def _():
            for u in range(UNROLL):
                start(first + u + depth, slot0 + u)

        return c

    lax.fori_loop(0, groups_of(n), body, 0)


def run_staged(n, codes, accs, tiles, other, tbuf, tsem, stage):
    run(
        n,
        lambda t, slot: start_tile(tiles, other, tbuf, tsem, codes[t], slot),
        lambda t, slot: wait_tile(tiles, tbuf, tsem, slot),
        lambda t, slot: stage[t],
        codes,
        accs,
        tbuf,
    )


def fill_stage(codes, first, last, ref, stage):
    def body(t, c):
        code = codes[t]
        stage[t] = ref[code >> 16, half_rows(code), :]
        return c

    lax.fori_loop(first, last, body, 0)


def total_of(accs, first, rows):
    total = accs[0, first : first + rows, :]
    for u in range(1, UNROLL):
        total = total + accs[u, first : first + rows, :]
    return total


def early_kernel(
    order, skip, pos, pos2, jtab, own, tiles, cached, block,
    acc, list1, off1, list2, off2, list3, off3, drift,
    clist, flags, accs, tbuf, sbuf, own_buf, tsem, ssem, osem,
):
    me = own[0]
    own_copy = pltpu.make_async_copy(cached.at[me], own_buf, osem)
    own_copy.start()

    def set_flag(r, c):
        flags[order[r]] = 1 - skip[r]
        return c

    lax.fori_loop(0, NB, set_flag, 0)

    def stale(j, n):
        clist[n] = (j << 4) | (pos[2 * j + 1] << 3) | pos[2 * j]
        return n + jnp.where((flags[j] == 0) & (j != me), 1, 0)

    nc = lax.fori_loop(0, NB, stale, 0)
    pad(clist, nc)

    def split(first, last, n, out):
        def build(t, n):
            j = jtab[t]
            fresh = flags[j]
            low = ((t - first) << 16) | (j << 4)
            out[n] = low | (pos[2 * j + 1] << 3) | pos[2 * j]
            n = n + jnp.where((fresh == 1) | (j == me), 1, 0)
            out[n] = low | (pos2[2 * j + 1] << 3) | 2 | pos2[2 * j]
            return n + fresh

        return lax.fori_loop(first, last, build, n)

    base = 0
    for group, (out, off) in enumerate(((list1, off1), (list2, off2), (list3, off3))):
        n = 0
        for p, size in enumerate(sizes(group)):
            off[p] = n
            n = split(base, base + size, n, out)
            base += size
        off[len(sizes(group))] = n
        pad(out, n)
    accs[...] = jnp.zeros_like(accs)

    def source_copy(t, slot):
        code = clist[t]
        return pltpu.make_async_copy(
            cached.at[(code >> 4) & 127, half_rows(code), :], sbuf.at[slot], ssem.at[slot]
        )

    def tile_copy(t, slot):
        return pltpu.make_async_copy(
            tiles.at[(clist[t] >> 4) & 127], tbuf.at[slot], tsem.at[slot]
        )

    def start(t, slot):
        tile_copy(t, slot).start()
        source_copy(t, slot).start()

    def wait(t, slot):
        tile_copy(t, slot).wait()
        source_copy(t, slot).wait()

    run(nc, start, wait, lambda t, slot: sbuf[slot], clist, accs, tbuf)
    acc[...] = total_of(accs, 0, ROWS)
    own_copy.wait()
    diff = block[0:ROWS, :].astype(jnp.float32) - own_buf[...].astype(jnp.float32)
    drift[...] = jnp.broadcast_to(jnp.sum(diff * diff, axis=0, keepdims=True), (8, W))


def add_pieces(codes, off, tiles, other, pieces, accs, tbuf, stage, tsem):
    accs[...] = jnp.zeros_like(accs)
    for p, ref in enumerate(pieces):
        fill_stage(codes, off[p], off[p + 1], ref, stage)
    run_staged(off[len(pieces)], codes, accs, tiles, other, tbuf, tsem, stage)


def mid_kernel(codes, off, acc_in, tiles, other, *rest):
    acc, accs, tbuf, stage, tsem = rest[-5:]
    add_pieces(codes, off, tiles, other, rest[:-5], accs, tbuf, stage, tsem)
    have = acc_in.shape[0]
    acc[0:have, :] = acc_in[...] + total_of(accs, 0, have)
    if have < 2 * ROWS:
        acc[have:, :] = total_of(accs, have, 2 * ROWS - have)


def late_kernel(codes, off, jtab, acc_in, tiles, other, *rest, drifts):
    if drifts:
        mine, theirs, accs, tbuf, stage, ext, tsem = rest[-7:]
        pieces = rest[:-7]
    else:
        mine, theirs, accs, tbuf, stage, tsem = rest[-6:]
        pieces = rest[:-6]
    late = len(sizes(2))
    add_pieces(codes, off, tiles, other, pieces[-late:], accs, tbuf, stage, tsem)
    mine[0:ROWS, :] = acc_in[0:ROWS, :] + total_of(accs, 0, ROWS)
    theirs[0:ROWS, :] = acc_in[ROWS:, :] + total_of(accs, ROWS, ROWS)
    if drifts:
        base = 0
        for ref in pieces:
            for s in range(ref.shape[0]):
                ext[jtab[base + s]] = ref[s, ROWS:, :].astype(jnp.float32)
            base += ref.shape[0]
        core = (jtab[0] >> 3) & 1
        total = jnp.zeros((16, W), jnp.float32)
        for hi in range(8):
            total = total + jnp.sum(ext[pl.ds(hi * 16 + core * 8, 8)], axis=0)
        mine[ROWS:, :] = total
        theirs[ROWS:, :] = total


def split3(row):
    hi = row.astype(jnp.bfloat16).astype(jnp.float32)
    mid = (row - hi).astype(jnp.bfloat16).astype(jnp.float32)
    return hi, mid, row - hi - mid


def finish_first_kernel(own, mine, theirs, drift_in, weight, cached, payload, own_buf, osem):
    own_copy = pltpu.make_async_copy(cached.at[own[0]], own_buf, osem)
    own_copy.start()
    total = mine[...] + theirs[...]
    hidden = jnp.maximum(
        jnp.dot(
            total.astype(jnp.bfloat16), weight[...], preferred_element_type=jnp.float32
        ),
        0.0,
    ).astype(jnp.bfloat16)
    payload[0:ROWS, :] = hidden
    own_copy.wait()
    diff = hidden.astype(jnp.float32) - own_buf[...].astype(jnp.float32)
    second = jnp.sum(diff * diff, axis=0, keepdims=True)
    row = lax.broadcasted_iota(jnp.int32, (16, W), 0)
    extra = jnp.zeros((16, W), jnp.float32)
    for k, part in enumerate(split3(drift_in[0:1, :]) + split3(second)):
        extra = jnp.where(row == k, jnp.broadcast_to(part, (16, W)), extra)
    payload[ROWS:, :] = extra.astype(jnp.bfloat16)


def finish_second_kernel(mine, theirs, weight, output, drift):
    total = mine[0:ROWS, :] + theirs[0:ROWS, :]
    output[...] = jnp.dot(
        total.astype(jnp.bfloat16), weight[...], preferred_element_type=jnp.float32
    ).astype(jnp.bfloat16)
    parts = mine[ROWS:, :] + theirs[ROWS:, :]
    cells = 1.0 / (NB * ROWS * W)
    drift[0] = jnp.sum(parts[0:3, :]) * cells
    drift[1] = jnp.sum(parts[3:6, :]) * cells


SMEM = pl.BlockSpec(memory_space=pltpu.SMEM)
VMEM = pl.BlockSpec(memory_space=pltpu.VMEM)
HBM = pl.BlockSpec(memory_space=pltpu.HBM)
ACCS = pltpu.VMEM((UNROLL, 5 * TS, W), jnp.float32)
BLOCK = pltpu.VMEM((ROWS, W), jnp.bfloat16)


def ring_of(depth):
    return [pltpu.VMEM((depth, TS, TS), jnp.bfloat16)]


def sems_of(depth):
    return pltpu.SemaphoreType.DMA((depth,))


def stage_of(blocks):
    return pltpu.VMEM((2 * blocks + UNROLL, TS, W), jnp.bfloat16)


def params(mib):
    return pltpu.CompilerParams(vmem_limit_bytes=mib * 1024 * 1024)


def cost(items):
    return pl.CostEstimate(
        flops=items * 2 * TS * TS * W, transcendentals=0, bytes_accessed=items * 196608
    )


def list_shapes():
    shapes = []
    for group in (0, 1, 2):
        shapes.append(jax.ShapeDtypeStruct((2 * sum(sizes(group)) + 8,), jnp.int32))
        shapes.append(jax.ShapeDtypeStruct((8,), jnp.int32))
    return shapes


def early(order, skip, pos, pos2, jtab, own, tiles, cached, block):
    return pl.pallas_call(
        early_kernel,
        out_shape=(
            jax.ShapeDtypeStruct((ROWS, W), jnp.float32),
            *list_shapes(),
            jax.ShapeDtypeStruct((8, W), jnp.float32),
        ),
        in_specs=[SMEM] * 6 + [HBM] * 2 + [VMEM],
        out_specs=(VMEM, *[SMEM] * 6, VMEM),
        scratch_shapes=[
            pltpu.SMEM((NB + 8,), jnp.int32),
            pltpu.SMEM((NB,), jnp.int32),
            ACCS,
            *ring_of(32),
            pltpu.VMEM((32, TS, W), jnp.bfloat16),
            BLOCK,
            sems_of(32),
            sems_of(32),
            pltpu.SemaphoreType.DMA,
        ],
        compiler_params=params(16),
        cost_estimate=cost(72),
        name="early_sum",
    )(order, skip, pos, pos2, jtab, own, tiles, cached, block)


def mid_sum(group, codes, off, acc, tiles, other, pieces):
    blocks = sum(sizes(group))
    return pl.pallas_call(
        mid_kernel,
        out_shape=jax.ShapeDtypeStruct((2 * ROWS, W), jnp.float32),
        in_specs=[SMEM] * 2 + [VMEM] + [HBM] * 2 + [VMEM] * len(pieces),
        out_specs=VMEM,
        scratch_shapes=[ACCS, *ring_of(32), stage_of(blocks), sems_of(32)],
        compiler_params=params(20),
        cost_estimate=cost(blocks),
    )(codes, off, acc, tiles, other, *pieces)


def late_sum(codes, off, jtab, acc, tiles, other, pieces, drifts):
    blocks = sum(sizes(2))
    rows = ROWS + 16 if drifts else ROWS
    extra = [pltpu.VMEM((NB, 16, W), jnp.float32)] if drifts else []
    return pl.pallas_call(
        functools.partial(late_kernel, drifts=drifts),
        out_shape=(jax.ShapeDtypeStruct((rows, W), jnp.float32),) * 2,
        in_specs=[SMEM] * 3 + [VMEM] + [HBM] * 2 + [VMEM] * len(pieces),
        out_specs=(VMEM, VMEM),
        scratch_shapes=[ACCS, *ring_of(32), stage_of(blocks), *extra, sems_of(32)],
        compiler_params=params(20),
        cost_estimate=cost(blocks),
        name="late_sum",
    )(codes, off, jtab, acc, tiles, other, *pieces)


def finish_first(own, mine, theirs, drift, weight, cached):
    return pl.pallas_call(
        finish_first_kernel,
        out_shape=jax.ShapeDtypeStruct((ROWS + 16, W), jnp.bfloat16),
        in_specs=[SMEM] + [VMEM] * 4 + [HBM],
        out_specs=VMEM,
        scratch_shapes=[BLOCK, pltpu.SemaphoreType.DMA],
        compiler_params=params(8),
        cost_estimate=cost(1),
        name="finish_first",
    )(own, mine, theirs, drift, weight, cached)


def finish_second(mine, theirs, weight):
    return pl.pallas_call(
        finish_second_kernel,
        out_shape=(
            jax.ShapeDtypeStruct((ROWS, W), jnp.bfloat16),
            jax.ShapeDtypeStruct((2,), jnp.float32),
        ),
        in_specs=[VMEM] * 3,
        out_specs=(VMEM, SMEM),
        compiler_params=params(8),
        cost_estimate=cost(1),
        name="finish_second",
    )(mine, theirs, weight)


def in_hbm(value):
    return pltpu.with_memory_space_constraint(value, pltpu.HBM)


def layer(block, order, skip, pos, pos2, jtab, own, tiles, other, cached, drifts):
    mid0, mid1, late = gather(block)
    acc, list1, off1, list2, off2, list3, off3, drift = early(
        order, skip, pos, pos2, jtab, own, tiles, cached, block
    )
    acc = mid_sum(0, list1, off1, acc, tiles, other, mid0)
    acc = mid_sum(1, list2, off2, acc, tiles, other, mid1)
    pieces = mid0 + mid1 + late if drifts else late
    mine, theirs = late_sum(list3, off3, jtab, acc, tiles, other, pieces, drifts)
    return mine, swap(theirs), drift


def on_device(features, cache_in, cache_hidden, tiles, tile_pos, order, skip, w_first, w_second):
    pos = tile_pos[0].reshape(2 * NB)
    own = lax.axis_index(AXES)[None].astype(jnp.int32)
    jtab = item_blocks()
    cache_in = in_hbm(cache_in.reshape(NB, ROWS, W))
    cache_hidden = in_hbm(cache_hidden.reshape(NB, ROWS, W))
    pos2 = swap(pos)
    other = in_hbm(swap(tiles[0]))
    tiles = in_hbm(tiles[0])
    mine, theirs, drift = layer(
        features, order[0], skip[0], pos, pos2, jtab, own, tiles, other, cache_in, False
    )
    payload = finish_first(own, mine, theirs, drift, w_first, cache_hidden)
    mine, theirs, _ = layer(
        payload, order[1], skip[1], pos, pos2, jtab, own, tiles, other, cache_hidden, True
    )
    return finish_second(mine, theirs, w_second)


def solution(mesh):
    split = Mesh(mesh.devices.reshape(2, 4, 2, 4, 2), AXES)
    both = AXES
    in_specs = (
        P(both, None),
        P(),
        P(),
        P(both, None, None, None),
        P(both, None, None),
        P(),
        P(),
        P(),
        P(),
    )
    out_specs = (P(both, None), P())
    return jax.shard_map(
        on_device, mesh=split, in_specs=in_specs, out_specs=out_specs, check_vma=False
    )
```

```python
import functools

import jax
import jax.numpy as jnp
from jax import lax
from jax.experimental import pallas as pl
from jax.experimental.pallas import tpu as pltpu
from jax.sharding import Mesh
from jax.sharding import PartitionSpec as P


AXES = ("ylo", "x", "core", "z", "yhi")
NB = 128
ROWS = 512
TS = 256
W = 128
UNROLL = 4
AX = ((1, 2, 0), (0, 2, 1))
QA = [(k, 0) for k in range(4)]
QB = [(k, 1) for k in range(4)] + [(k, 3) for k in range(4)]
QC = [(k, 2) for k in range(4)]
GROUPS = (
    ((QA, 0), (QA, 1), (QA, 3), (QA, 2), (QB, 0), (QC, 0)),
    ((QB, 1), (QB, 3), (QC, 1), (QC, 3)),
    ((QB[:4], 2), (QB[4:], 2), (QC, 2)),
)


def sizes(group):
    return [len(q) for q, _ in GROUPS[group]]


def coords(i):
    return [(i // 16) % 4, (i % 2) * 2 + i // 64, (i // 2) % 4, (i // 8) % 2]


def block_id(x, y, z, core):
    return (y % 2) * 64 + x * 16 + core * 8 + z * 2 + y // 2


def stage_perm(stage, shift):
    pairs = []
    for i in range(NB):
        c = coords(i)
        a = AX[c[3]][stage]
        c[a] = (c[a] + shift) % 4
        pairs.append((i, block_id(*c)))
    return pairs


PERM = {(s, k): stage_perm(s, k) for s in range(3) for k in (1, 2, 3)}
SWAP = [(i, i ^ 8) for i in range(NB)]


def shift(value, stage, k):
    return lax.ppermute(value, AXES, PERM[(stage, k)])


def swap(value):
    return lax.ppermute(value, AXES, SWAP)


def gather(block):
    s1 = block[None]
    qa = jnp.concatenate([s1] + [shift(s1, 0, k) for k in (1, 2, 3)], 0)
    q1, q3, q2 = (shift(qa, 1, k) for k in (1, 3, 2))
    ap = shift(qa, 2, 1)
    am = shift(qa, 2, 3)
    ao = shift(qa, 2, 2)
    qb = jnp.concatenate([q1, q3], 0)
    bp = shift(qb, 2, 1)
    bm = shift(qb, 2, 3)
    cp = shift(q2, 2, 1)
    cm = shift(q2, 2, 3)
    co = shift(q2, 2, 2)
    fm = shift(bm[:4], 2, 3)
    fp = shift(bp[4:], 2, 1)
    return [qa, ap, am, ao, qb, q2], [bp, bm, cp, cm], [fm, fp, co]


def item_blocks():
    k1, k2, k3 = [], [], []
    for group in GROUPS:
        for slots, third in group:
            for first, second in slots:
                k1.append(first)
                k2.append(second)
                k3.append(third)
    k1, k2, k3 = (jnp.array(v, jnp.int32) for v in (k1, k2, k3))
    core = lax.axis_index("core")
    y = lax.axis_index("yhi") * 2 + lax.axis_index("ylo")
    zero = core == 0
    bx = (lax.axis_index("x") - jnp.where(zero, k3, k1)) & 3
    by = (y - jnp.where(zero, k1, k3)) & 3
    bz = (lax.axis_index("z") - k2) & 3
    return (by & 1) * 64 + bx * 16 + core * 8 + bz * 2 + (by >> 1)


PADDING = 4


def groups_of(n):
    return (n + (UNROLL - 1)) // UNROLL


def pad(ref, n):
    for u in range(UNROLL - 1):
        ref[n + u] = PADDING


def half_rows(code):
    return pl.ds(((code >> 3) & 1) * TS, TS)


def start_tile(tiles, other, tbuf, tsem, code, slot):
    block = (code >> 4) & 127
    theirs = (code >> 1) & 1

    @pl.when(theirs == 0)
    def _():
        pltpu.make_async_copy(tiles.at[block], tbuf.at[slot], tsem.at[slot]).start()

    @pl.when(theirs == 1)
    def _():
        pltpu.make_async_copy(other.at[block], tbuf.at[slot], tsem.at[slot]).start()


def wait_tile(tiles, tbuf, tsem, slot):
    pltpu.make_async_copy(tiles.at[0], tbuf.at[slot], tsem.at[slot]).wait()


def steps_of(n):
    return groups_of(n) * UNROLL


def prime(n, start, depth):
    def body(t, c):
        start(t, t)
        return c

    lax.fori_loop(0, jnp.minimum(steps_of(n), depth), body, 0)


def run(n, start, wait, source, codes, accs, tbuf):
    depth = tbuf.shape[0]
    total = steps_of(n)

    def body(g, c):
        first = g * UNROLL
        slot0 = first & (depth - 1)
        for u in range(UNROLL):
            wait(first + u, slot0 + u)
        for u in range(UNROLL):
            rows = pl.ds((codes[first + u] & 7) * TS, TS)
            accs[u, rows, :] += jnp.dot(
                tbuf[slot0 + u],
                source(first + u, slot0 + u),
                preferred_element_type=jnp.float32,
            )

        @pl.when(first + depth < total)
        def _():
            for u in range(UNROLL):
                start(first + u + depth, slot0 + u)

        return c

    lax.fori_loop(0, groups_of(n), body, 0)


def fill_stage(codes, first, last, ref, stage):
    def body(t, c):
        code = codes[t]
        stage[t] = ref[code >> 16, half_rows(code), :]
        return c

    lax.fori_loop(first, last, body, 0)


def total_of(accs, first, rows):
    total = accs[0, first : first + rows, :]
    for u in range(1, UNROLL):
        total = total + accs[u, first : first + rows, :]
    return total


def plan_kernel(order, skip, pos, pos2, jtab, own, *outs):
    flags = outs[-1]
    me = own[0]
    for layer in range(2):
        clist, nc, *lists = outs[layer * 8 : layer * 8 + 8]

        def set_flag(r, c):
            flags[order[layer * NB + r]] = 1 - skip[layer * NB + r]
            return c

        lax.fori_loop(0, NB, set_flag, 0, unroll=8)

        def stale(j, n):
            clist[n] = (j << 4) | (pos[2 * j + 1] << 3) | pos[2 * j]
            return n + jnp.where((flags[j] == 0) & (j != me), 1, 0)

        n = lax.fori_loop(0, NB, stale, 0, unroll=8)
        nc[0] = n
        pad(clist, n)
        base = 0
        for group in range(3):
            out, off = lists[2 * group], lists[2 * group + 1]
            n = 0
            for p, size in enumerate(sizes(group)):
                off[p] = n

                def build(s, n):
                    j = jtab[base + s]
                    fresh = flags[j]
                    low = (s << 16) | (j << 4)
                    out[n] = low | (pos[2 * j + 1] << 3) | pos[2 * j]
                    n = n + jnp.where((fresh == 1) | (j == me), 1, 0)
                    out[n] = low | (pos2[2 * j + 1] << 3) | 2 | pos2[2 * j]
                    return n + fresh

                n = lax.fori_loop(0, size, build, n, unroll=4)
                base += size
            off[len(sizes(group))] = n
            pad(out, n)


def early_kernel(
    own, clist, nc, tiles, cached, block, acc, drift, accs, tbuf, sbuf, own_buf, tsem, ssem, osem
):
    def source_copy(t, slot):
        code = clist[t]
        return pltpu.make_async_copy(
            cached.at[(code >> 4) & 127, half_rows(code), :], sbuf.at[slot], ssem.at[slot]
        )

    def tile_copy(t, slot):
        return pltpu.make_async_copy(
            tiles.at[(clist[t] >> 4) & 127], tbuf.at[slot], tsem.at[slot]
        )

    def start(t, slot):
        tile_copy(t, slot).start()
        source_copy(t, slot).start()

    def wait(t, slot):
        tile_copy(t, slot).wait()
        source_copy(t, slot).wait()

    n = nc[0]
    prime(n, start, tbuf.shape[0])
    own_copy = pltpu.make_async_copy(cached.at[own[0]], own_buf, osem)
    own_copy.start()
    accs[:, 0:ROWS, :] = jnp.zeros((UNROLL, ROWS, W), jnp.float32)
    run(n, start, wait, lambda t, slot: sbuf[slot], clist, accs, tbuf)
    acc[...] = total_of(accs, 0, ROWS)
    own_copy.wait()
    diff = block[0:ROWS, :].astype(jnp.float32) - own_buf[...].astype(jnp.float32)
    drift[...] = jnp.broadcast_to(jnp.sum(diff * diff, axis=0, keepdims=True), (8, W))


def add_pieces(
    codes, off, tiles, other, pieces, accs, tbuf, stage, tsem, then=lambda: None
):
    n = off[len(pieces)]

    def start(t, slot):
        start_tile(tiles, other, tbuf, tsem, codes[t], slot)

    prime(n, start, tbuf.shape[0])
    then()
    accs[:, 0 : 2 * ROWS, :] = jnp.zeros((UNROLL, 2 * ROWS, W), jnp.float32)
    for p, ref in enumerate(pieces):
        fill_stage(codes, off[p], off[p + 1], ref, stage)
    run(
        n,
        start,
        lambda t, slot: wait_tile(tiles, tbuf, tsem, slot),
        lambda t, slot: stage[t],
        codes,
        accs,
        tbuf,
    )


def mid_kernel(codes, off, acc_in, tiles, other, *rest):
    acc, accs, tbuf, stage, tsem = rest[-5:]
    add_pieces(codes, off, tiles, other, rest[:-5], accs, tbuf, stage, tsem)
    have = acc_in.shape[0]
    acc[0:have, :] = acc_in[...] + total_of(accs, 0, have)
    if have < 2 * ROWS:
        acc[have:, :] = total_of(accs, have, 2 * ROWS - have)


def mid_fetch_kernel(next_codes, next_off, codes, off, acc_in, tiles, other, *rest):
    acc, fetched, accs, tbuf, stage, tsem, fsem = rest[-7:]
    n = steps_of(next_off[len(sizes(2))])

    def start(t, c):
        start_tile(tiles, other, fetched, fsem, next_codes[t], t)
        return c

    def wait(t, c):
        wait_tile(tiles, fetched, fsem, t)
        return c

    add_pieces(
        codes, off, tiles, other, rest[:-7], accs, tbuf, stage, tsem,
        lambda: lax.fori_loop(0, n, start, 0),
    )
    acc[...] = acc_in[...] + total_of(accs, 0, 2 * ROWS)
    lax.fori_loop(0, n, wait, 0)


def late_kernel(codes, off, jtab, acc_in, tiles, *rest, drifts):
    if drifts:
        mine, theirs, accs, stage, ext = rest[-5:]
        pieces = rest[:-5]
    else:
        mine, theirs, accs, stage = rest[-4:]
        pieces = rest[:-4]
    accs[:, 0 : 2 * ROWS, :] = jnp.zeros((UNROLL, 2 * ROWS, W), jnp.float32)
    late = pieces[-len(sizes(2)) :]
    for p, ref in enumerate(late):
        fill_stage(codes, off[p], off[p + 1], ref, stage)

    def body(g, c):
        for u in range(UNROLL):
            t = g * UNROLL + u
            accs[u, pl.ds((codes[t] & 7) * TS, TS), :] += jnp.dot(
                tiles[t], stage[t], preferred_element_type=jnp.float32
            )
        return c

    lax.fori_loop(0, groups_of(off[len(late)]), body, 0)
    mine[0:ROWS, :] = acc_in[0:ROWS, :] + total_of(accs, 0, ROWS)
    theirs[0:ROWS, :] = acc_in[ROWS:, :] + total_of(accs, ROWS, ROWS)
    if drifts:
        base = 0
        for ref in pieces:
            for s in range(ref.shape[0]):
                ext[jtab[base + s]] = ref[s, ROWS:, :].astype(jnp.float32)
            base += ref.shape[0]
        core = (jtab[0] >> 3) & 1
        total = jnp.zeros((16, W), jnp.float32)
        for hi in range(8):
            total = total + jnp.sum(ext[pl.ds(hi * 16 + core * 8, 8)], axis=0)
        mine[ROWS:, :] = total
        theirs[ROWS:, :] = total


def split3(row):
    hi = row.astype(jnp.bfloat16).astype(jnp.float32)
    mid = (row - hi).astype(jnp.bfloat16).astype(jnp.float32)
    return hi, mid, row - hi - mid


def finish_first_kernel(own, mine, theirs, drift_in, weight, cached, payload, own_buf, osem):
    own_copy = pltpu.make_async_copy(cached.at[own[0]], own_buf, osem)
    own_copy.start()
    total = mine[...] + theirs[...]
    hidden = jnp.maximum(
        jnp.dot(
            total.astype(jnp.bfloat16), weight[...], preferred_element_type=jnp.float32
        ),
        0.0,
    ).astype(jnp.bfloat16)
    payload[0:ROWS, :] = hidden
    own_copy.wait()
    diff = hidden.astype(jnp.float32) - own_buf[...].astype(jnp.float32)
    second = jnp.sum(diff * diff, axis=0, keepdims=True)
    row = lax.broadcasted_iota(jnp.int32, (16, W), 0)
    extra = jnp.zeros((16, W), jnp.float32)
    for k, part in enumerate(split3(drift_in[0:1, :]) + split3(second)):
        extra = jnp.where(row == k, jnp.broadcast_to(part, (16, W)), extra)
    payload[ROWS:, :] = extra.astype(jnp.bfloat16)


def finish_second_kernel(mine, theirs, weight, output, drift):
    total = mine[0:ROWS, :] + theirs[0:ROWS, :]
    output[...] = jnp.dot(
        total.astype(jnp.bfloat16), weight[...], preferred_element_type=jnp.float32
    ).astype(jnp.bfloat16)
    parts = mine[ROWS:, :] + theirs[ROWS:, :]
    cells = 1.0 / (NB * ROWS * W)
    drift[0] = jnp.sum(parts[0:3, :]) * cells
    drift[1] = jnp.sum(parts[3:6, :]) * cells


SMEM = pl.BlockSpec(memory_space=pltpu.SMEM)
VMEM = pl.BlockSpec(memory_space=pltpu.VMEM)
HBM = pl.BlockSpec(memory_space=pltpu.HBM)
ACCS = pltpu.VMEM((UNROLL, 5 * TS, W), jnp.float32)
BLOCK = pltpu.VMEM((ROWS, W), jnp.bfloat16)


def ring_of(depth):
    return [pltpu.VMEM((depth, TS, TS), jnp.bfloat16)]


def sems_of(depth):
    return pltpu.SemaphoreType.DMA((depth,))


def stage_of(blocks):
    return pltpu.VMEM((2 * blocks + UNROLL, TS, W), jnp.bfloat16)


def params(mib):
    return pltpu.CompilerParams(vmem_limit_bytes=mib * 1024 * 1024)


def cost(items):
    return pl.CostEstimate(
        flops=items * 2 * TS * TS * W, transcendentals=0, bytes_accessed=items * 196608
    )


def plan(order, skip, pos, pos2, jtab, own):
    def ints(n):
        return jax.ShapeDtypeStruct((n,), jnp.int32)

    shapes = [ints(NB + 8), ints(1)]
    for group in range(3):
        shapes += [ints(2 * sum(sizes(group)) + 8), ints(8)]
    lists = pl.pallas_call(
        plan_kernel,
        out_shape=tuple(shapes * 2),
        in_specs=[SMEM] * 6,
        out_specs=tuple([SMEM] * 16),
        scratch_shapes=[pltpu.SMEM((NB,), jnp.int32)],
        compiler_params=params(2),
        cost_estimate=cost(24),
        name="plan",
    )(order, skip, pos, pos2, jtab, own)
    return lists[:8], lists[8:]


def early(own, clist, nc, tiles, cached, block):
    return pl.pallas_call(
        early_kernel,
        out_shape=(
            jax.ShapeDtypeStruct((ROWS, W), jnp.float32),
            jax.ShapeDtypeStruct((8, W), jnp.float32),
        ),
        in_specs=[SMEM] * 3 + [HBM] * 2 + [VMEM],
        out_specs=(VMEM, VMEM),
        scratch_shapes=[
            ACCS,
            *ring_of(32),
            pltpu.VMEM((32, TS, W), jnp.bfloat16),
            BLOCK,
            sems_of(32),
            sems_of(32),
            pltpu.SemaphoreType.DMA,
        ],
        compiler_params=params(16),
        cost_estimate=cost(72),
        name="early_sum",
    )(own, clist, nc, tiles, cached, block)


def mid_sum(group, codes, off, acc, tiles, other, pieces):
    blocks = sum(sizes(group))
    return pl.pallas_call(
        mid_kernel,
        out_shape=jax.ShapeDtypeStruct((2 * ROWS, W), jnp.float32),
        in_specs=[SMEM] * 2 + [VMEM] + [HBM] * 2 + [VMEM] * len(pieces),
        out_specs=VMEM,
        scratch_shapes=[ACCS, *ring_of(32), stage_of(blocks), sems_of(32)],
        compiler_params=params(20),
        cost_estimate=cost(blocks),
    )(codes, off, acc, tiles, other, *pieces)


def mid_fetch(next_codes, next_off, codes, off, acc, tiles, other, pieces):
    blocks = sum(sizes(1))
    ahead = 2 * sum(sizes(2)) + UNROLL
    return pl.pallas_call(
        mid_fetch_kernel,
        out_shape=(
            jax.ShapeDtypeStruct((2 * ROWS, W), jnp.float32),
            jax.ShapeDtypeStruct((ahead, TS, TS), jnp.bfloat16),
        ),
        in_specs=[SMEM] * 4 + [VMEM] + [HBM] * 2 + [VMEM] * len(pieces),
        out_specs=(VMEM, VMEM),
        scratch_shapes=[
            ACCS, *ring_of(32), stage_of(blocks), sems_of(32), sems_of(ahead)
        ],
        compiler_params=params(24),
        cost_estimate=cost(blocks),
        name="mid1_sum",
    )(next_codes, next_off, codes, off, acc, tiles, other, *pieces)


def late_sum(codes, off, jtab, acc, tiles, pieces, drifts):
    blocks = sum(sizes(2))
    rows = ROWS + 16 if drifts else ROWS
    extra = [pltpu.VMEM((NB, 16, W), jnp.float32)] if drifts else []
    return pl.pallas_call(
        functools.partial(late_kernel, drifts=drifts),
        out_shape=(jax.ShapeDtypeStruct((rows, W), jnp.float32),) * 2,
        in_specs=[SMEM] * 3 + [VMEM] * (2 + len(pieces)),
        out_specs=(VMEM, VMEM),
        scratch_shapes=[ACCS, stage_of(blocks), *extra],
        compiler_params=params(16),
        cost_estimate=cost(blocks),
        name="late_sum",
    )(codes, off, jtab, acc, tiles, *pieces)


def finish_first(own, mine, theirs, drift, weight, cached):
    return pl.pallas_call(
        finish_first_kernel,
        out_shape=jax.ShapeDtypeStruct((ROWS + 16, W), jnp.bfloat16),
        in_specs=[SMEM] + [VMEM] * 4 + [HBM],
        out_specs=VMEM,
        scratch_shapes=[BLOCK, pltpu.SemaphoreType.DMA],
        compiler_params=params(8),
        cost_estimate=cost(1),
        name="finish_first",
    )(own, mine, theirs, drift, weight, cached)


def finish_second(mine, theirs, weight):
    return pl.pallas_call(
        finish_second_kernel,
        out_shape=(
            jax.ShapeDtypeStruct((ROWS, W), jnp.bfloat16),
            jax.ShapeDtypeStruct((2,), jnp.float32),
        ),
        in_specs=[VMEM] * 3,
        out_specs=(VMEM, SMEM),
        compiler_params=params(8),
        cost_estimate=cost(1),
        name="finish_second",
    )(mine, theirs, weight)


def in_hbm(value):
    return pltpu.with_memory_space_constraint(value, pltpu.HBM)


def layer(block, lists, jtab, own, tiles, other, cached, drifts):
    clist, nc, list0, off0, list1, off1, list2, off2 = lists
    mid0, mid1, late = gather(block)
    acc, drift = early(own, clist, nc, tiles, cached, block)
    acc = mid_sum(0, list0, off0, acc, tiles, other, mid0)
    acc, fetched = mid_fetch(list2, off2, list1, off1, acc, tiles, other, mid1)
    pieces = mid0 + mid1 + late if drifts else late
    mine, theirs = late_sum(list2, off2, jtab, acc, fetched, pieces, drifts)
    return mine, swap(theirs), drift


def on_device(features, cache_in, cache_hidden, tiles, tile_pos, order, skip, w_first, w_second):
    pos = tile_pos[0].reshape(2 * NB)
    own = lax.axis_index(AXES)[None].astype(jnp.int32)
    jtab = item_blocks()
    cache_in = in_hbm(cache_in.reshape(NB, ROWS, W))
    cache_hidden = in_hbm(cache_hidden.reshape(NB, ROWS, W))
    pos2 = swap(pos)
    other = in_hbm(swap(tiles[0]))
    tiles = in_hbm(tiles[0])
    first, second = plan(order.reshape(2 * NB), skip.reshape(2 * NB), pos, pos2, jtab, own)
    mine, theirs, drift = layer(
        features, first, jtab, own, tiles, other, cache_in, False
    )
    payload = finish_first(own, mine, theirs, drift, w_first, cache_hidden)
    mine, theirs, _ = layer(
        payload, second, jtab, own, tiles, other, cache_hidden, True
    )
    return finish_second(mine, theirs, w_second)


def solution(mesh):
    split = Mesh(mesh.devices.reshape(2, 4, 2, 4, 2), AXES)
    both = AXES
    in_specs = (
        P(both, None),
        P(),
        P(),
        P(both, None, None, None),
        P(both, None, None),
        P(),
        P(),
        P(),
        P(),
    )
    out_specs = (P(both, None), P())
    return jax.shard_map(
        on_device, mesh=split, in_specs=in_specs, out_specs=out_specs, check_vma=False
    )
```
